32 devices in a mesh: gx: 4 (over x, core), gy: 2 (over y), gz: 4 (over z).
Axes of the slice: x: 2, y: 2, z: 4, core: 2. Of those that a mesh axis runs over, the one named last changes fastest.
Arguments:
- velocity: float32 [3, 128, 192, 1024], P(None, 'gx', 'gy', 'gz'), may hold values from -6 to 6
Outputs:
- magnitude: float32 [128, 192, 1024], P('gx', ('gy', 'gz'))
- level_one: float32 [64, 96, 512], P('gx', 'gy')
- level_two: float32 [32, 48, 256], P('gx', 'gy')
- level_three: float32 [16, 24, 128], P('gx', 'gy')
- level_four: float32 [8, 12, 64], P('gx', 'gy')
- level_five: float32 [4, 6, 32], P('gx', 'gy')
The draws below stay inside these ranges and needn't reach their ends.
All inputs are finite; a program needn't handle non-finite values.
Results may differ from the reference program's by a relative error of at most 0.000075.
Values sent between devices are 32-bit elements; how exact they have to be, the bound alone decides.
A program may use at most 256 MiB of HBM per device.

```python
import jax
import jax.numpy as jnp
from jax import lax

NX = 128
NY = 192
NZ = 1024


def shard_levels(stream_key, extent, cuts, least, top_value):
    loudness, own = 1.0, jax.random.fold_in(stream_key, 6)
    for axis_at, blocks in cuts:
        steps = jnp.exp(jax.random.uniform(jax.random.fold_in(own, axis_at), (blocks,), jnp.float32, least / len(cuts), top_value / len(cuts)))
        loudness = loudness * jnp.repeat(steps, extent[axis_at] // blocks).reshape([-1 if axis == axis_at else 1 for axis in range(len(extent))])
    return loudness


def normal_values(own_key, extent, scale, limit, split=(), held_as=jnp.bfloat16):
    level = shard_levels(own_key, extent, split, -0.22, 0.18) if split else 1.0
    array = jax.random.normal(own_key, extent, jnp.float32) * scale * level
    return jnp.minimum(jnp.maximum(array, -limit), limit).astype(held_as)


def setup_inputs(seed: int = 0) -> dict:
    streams_of = jax.random.split(jax.random.key(seed), 2)
    velocity = normal_values(streams_of[0], (3, NX, NY, NZ), 1.0, 6.0, ((1, 4), (2, 2), (3, 4)), jnp.float32)
    return {"velocity": velocity}


def central(field, axis):
    return (jnp.roll(field, -1, axis) - jnp.roll(field, 1, axis)) * 0.5

def pooled(field):
    rows, cols, depth = field.shape
    blocks = field.reshape(rows // 2, 2, cols // 2, 2, depth // 2, 2)
    return lax.optimization_barrier(jnp.mean(blocks, axis=(1, 3, 5)))

def reference(velocity):
    speed_u = velocity[0]
    speed_v = velocity[1]
    speed_w = velocity[2]
    curl_first = central(speed_w, 1) - central(speed_v, 2)
    curl_second = central(speed_u, 2) - central(speed_w, 0)
    curl_third = central(speed_v, 0) - central(speed_u, 1)
    magnitude = jnp.sqrt(1.0 + curl_first * curl_first + curl_second * curl_second + curl_third * curl_third)
    level_one = pooled(magnitude)
    level_two = pooled(level_one)
    level_three = pooled(level_two)
    level_four = pooled(level_three)
    level_five = pooled(level_four)
    return (magnitude, level_one, level_two, level_three, level_four, level_five)
```

```python
import functools

import jax
import jax.numpy as jnp
from jax import lax
from jax.experimental import pallas as pl
from jax.experimental.pallas import tpu as pltpu
from jax.sharding import PartitionSpec as P

MESH = pl.DeviceIdType.MESH
LANES = 128
LOADS = 4


def remote(src, dst, send, recv, device):
    return pltpu.make_async_remote_copy(
        src_ref=src, dst_ref=dst, send_sem=send, recv_sem=recv, device_id=device, device_id_type=MESH
    )


def halves(size, along):
    shape = (size, size // 2) if along else (size // 2, size)
    fine = lax.broadcasted_iota(jnp.int32, shape, 1 - along)
    coarse = lax.broadcasted_iota(jnp.int32, shape, along)
    return jnp.where(fine // 2 == coarse, 1.0, 0.0).astype(jnp.float32)


def dot(a, b):
    return jnp.dot(a, b, precision=lax.Precision.HIGHEST, preferred_element_type=jnp.float32)


def merge(summed):
    rows, depth = summed.shape
    across = dot(summed, halves(depth, 1))
    return dot(halves(rows, 0), across) * 0.125


def kernel(
    sizes, vel_hbm, pencil, one_out, two, three, four, five,
    vel, ypack, yhalo, zpack, zhalo, stage, one, own_one,
    load_sem, xs_sem, xr_sem, ys_sem, yr_sem, zs_sem, zr_sem,
    as_sem, ar_sem, own_sem, up_sem, down_sem, one_sem, store_sem,
):
    nx, ny, nz = sizes
    gx, gy, me = lax.axis_index("gx"), lax.axis_index("gy"), lax.axis_index("gz")
    _, planes, cols, depth = vel_hbm.shape
    rows = cols // nz
    half = depth // 2

    def at(dx=0, dy=0, dz=0):
        return (lax.rem(gx + dx + nx, nx), lax.rem(gy + dy + ny, ny), lax.rem(me + dz + nz, nz))

    barrier = pltpu.get_barrier_semaphore()
    friends = [at(dx=1), at(dx=-1), at(dy=1), at(dy=-1)] + [at(dz=d) for d in range(1, nz)]
    for friend in friends:
        pl.semaphore_signal(barrier, inc=1, device_id=friend, device_id_type=MESH)

    step = planes // LOADS
    loads = []
    for k in range(LOADS):
        loads.append(pltpu.make_async_copy(
            vel_hbm.at[:, pl.ds(k * step, step)], vel.at[:, pl.ds(1 + k * step, step)], load_sem.at[k]))
        loads[-1].start()
    pl.semaphore_wait(barrier, len(friends))

    xcopies = [
        remote(vel_hbm.at[pl.ds(1, 2), planes - 1], vel.at[pl.ds(1, 2), 0], xs_sem.at[0], xr_sem.at[0], at(dx=1)),
        remote(vel_hbm.at[pl.ds(1, 2), 0], vel.at[pl.ds(1, 2), planes + 1], xs_sem.at[1], xr_sem.at[1], at(dx=-1)),
    ]
    for copy in xcopies:
        copy.start()

    lane = lax.broadcasted_iota(jnp.int32, (cols, LANES), 1)

    def pack(x, carry):
        first, last = carry
        for c in range(2):
            first = jnp.where(lane == c * planes + x, vel[c, x + 1, :, 0:1], first)
            last = jnp.where(lane == c * planes + x, vel[c, x + 1, :, depth - 1:depth], last)
            ypack[0, c, pl.ds(x, 1), :] = vel[2 * c, x + 1, 0:1, :]
            ypack[1, c, pl.ds(x, 1), :] = vel[2 * c, x + 1, cols - 1:cols, :]
        return first, last

    carry = (jnp.zeros((cols, LANES), jnp.float32), jnp.zeros((cols, LANES), jnp.float32))
    for k in range(LOADS):
        loads[k].wait()
        carry = lax.fori_loop(k * step, (k + 1) * step, pack, carry)
    zpack[0], zpack[1] = carry
    side = [
        remote(ypack.at[1], yhalo.at[0], ys_sem.at[0], yr_sem.at[0], at(dy=1)),
        remote(ypack.at[0], yhalo.at[1], ys_sem.at[1], yr_sem.at[1], at(dy=-1)),
        remote(zpack.at[1], zhalo.at[0], zs_sem.at[0], zr_sem.at[0], at(dz=1)),
        remote(zpack.at[0], zhalo.at[1], zs_sem.at[1], zr_sem.at[1], at(dz=-1)),
    ]
    for copy in side:
        copy.start()
    for copy in xcopies + side:
        copy.wait_recv()

    row = lax.broadcasted_iota(jnp.int32, (cols, depth), 0)
    deep = lax.broadcasted_iota(jnp.int32, (cols, depth), 1)

    def second(c, x):
        field = vel[2 * c, x + 1]
        ahead = jnp.where(row == cols - 1, yhalo[1, c, pl.ds(x, 1), :], pltpu.roll(field, cols - 1, 0))
        behind = jnp.where(row == 0, yhalo[0, c, pl.ds(x, 1), :], pltpu.roll(field, 1, 0))
        return ahead - behind

    def third(c, x):
        field = vel[c, x + 1]
        shift = LANES - (c * planes + x)
        shift = jnp.where(shift == LANES, 0, shift)
        after = pltpu.roll(zhalo[1], shift, 1)[:, 0:1]
        before = pltpu.roll(zhalo[0], shift, 1)[:, 0:1]
        ahead = jnp.where(deep == depth - 1, after, pltpu.roll(field, depth - 1, 1))
        behind = jnp.where(deep == 0, before, pltpu.roll(field, 1, 1))
        return ahead - behind

    def magnitude(x):
        total = second(1, x) - third(1, x)
        total = total * total
        part = third(0, x) - (vel[2, x + 2] - vel[2, x])
        total = total + part * part
        part = (vel[1, x + 2] - vel[1, x]) - second(0, x)
        total = total + part * part
        return jnp.sqrt(1.0 + 0.25 * total)

    def block(target, first, count):
        here = pl.ds(pl.multiple_of(me * depth, LANES), depth)
        return remote(
            stage.at[target, pl.ds(first, count)], pencil.at[pl.ds(first, count), :, here],
            as_sem.at[target], ar_sem.at[me], (gx, gy, target))

    def near(first):
        @pl.when(me < nz - 1)
        def _():
            block(me + 1, first, 2).start()

        @pl.when(me > 0)
        def _():
            block(me - 1, first, 2).start()

    def pair(i, carry):
        x = 2 * i
        summed = None
        for k in range(2):
            value = magnitude(x + k)
            for q in range(nz):
                stage[q, x + k] = value[q * rows:(q + 1) * rows, :]
            summed = value if summed is None else summed + value

        @pl.when(i > 0)
        def _():
            near(x - 2)
        own_one[i] = merge(summed)
        return carry

    lax.fori_loop(0, planes // 2, pair, 0)
    near(planes - 2)

    def lanes_of(piece):
        return one.at[:, :, pl.ds(pl.multiple_of(piece * half, LANES), half)]

    def hop(piece, source, up):
        return remote(
            source, lanes_of(piece), (up_sem if up else down_sem).at[piece], one_sem.at[piece],
            (gx, gy, jnp.minimum(me + 1, nz - 1) if up else jnp.maximum(me - 1, 0)))

    @pl.when(me < nz - 1)
    def _():
        hop(me, own_one, True).start()

    @pl.when(me > 0)
    def _():
        hop(me, own_one, False).start()

    def far():
        for d in range(2, nz):
            @pl.when(me + d < nz)
            def _():
                block(me + d, 0, planes).start()

            @pl.when(me - d >= 0)
            def _():
                block(me - d, 0, planes).start()

    end = jnp.logical_or(me == 0, me == nz - 1)

    @pl.when(end)
    def _():
        far()
    keep = pltpu.make_async_copy(
        stage.at[me], pencil.at[:, :, pl.ds(pl.multiple_of(me * depth, LANES), depth)], own_sem.at[0])
    keep.start()
    mine = pltpu.make_async_copy(own_one, lanes_of(me), own_sem.at[1])
    mine.start()

    for k in range(1, nz):
        @pl.when(me - k >= 0)
        def _():
            hop(me - k, own_one, True).wait_recv()

            @pl.when(me < nz - 1)
            def _():
                hop(me - k, lanes_of(me - k), True).start()

        @pl.when(me + k < nz)
        def _():
            hop(me + k, own_one, False).wait_recv()

            @pl.when(me > 0)
            def _():
                hop(me + k, lanes_of(me + k), False).start()
        if k == 1:
            @pl.when(jnp.logical_not(end))
            def _():
                far()
    mine.wait()

    store = pltpu.make_async_copy(one, one_out, store_sem)
    store.start()

    def second_level(i, carry):
        two[i] = merge(one[2 * i] + one[2 * i + 1])
        return carry

    lax.fori_loop(0, two.shape[0], second_level, 0)
    for fine, coarse in ((two, three), (three, four), (four, five)):
        for i in range(coarse.shape[0]):
            coarse[i] = merge(fine[2 * i] + fine[2 * i + 1])
    store.wait()
    keep.wait()
    for copy in xcopies + side:
        copy.wait_send()
    for p in range(nz):
        @pl.when(jnp.logical_and(p <= me, me < nz - 1))
        def _():
            hop(p, own_one, True).wait_send()

        @pl.when(jnp.logical_and(p >= me, me > 0))
        def _():
            hop(p, own_one, False).wait_send()
    for p in range(nz):
        @pl.when(p != me)
        def _():
            block(p, 0, planes).wait_send()
            there = pl.ds(p * depth, depth)
            remote(stage.at[p], pencil.at[:, :, there], as_sem.at[p], ar_sem.at[p], (gx, gy, p)).wait_recv()


def on_device(velocity):
    nx, ny, nz = (lax.axis_size(a) for a in ("gx", "gy", "gz"))
    _, planes, cols, depth = velocity.shape
    full = depth * nz
    f32 = jnp.float32

    def level(k):
        return jax.ShapeDtypeStruct((planes >> k, cols >> k, full >> k), f32)

    vmem = pl.BlockSpec(memory_space=pltpu.VMEM)
    anywhere = pl.BlockSpec(memory_space=pl.ANY)
    dma = pltpu.SemaphoreType.DMA
    return pl.pallas_call(
        functools.partial(kernel, (nx, ny, nz)),
        out_shape=(jax.ShapeDtypeStruct((planes, cols // nz, full), f32),) + tuple(level(k) for k in range(1, 6)),
        in_specs=[anywhere],
        out_specs=(anywhere, anywhere, vmem, vmem, vmem, vmem),
        scratch_shapes=[
            pltpu.VMEM((3, planes + 2, cols, depth), f32),
            pltpu.VMEM((2, 2, planes, depth), f32),
            pltpu.VMEM((2, 2, planes, depth), f32),
            pltpu.VMEM((2, cols, LANES), f32),
            pltpu.VMEM((2, cols, LANES), f32),
            pltpu.VMEM((nz, planes, cols // nz, depth), f32),
            pltpu.VMEM((planes // 2, cols // 2, full // 2), f32),
            pltpu.VMEM((planes // 2, cols // 2, depth // 2), f32),
            dma((LOADS,)), dma((2,)), dma((2,)), dma((2,)), dma((2,)), dma((2,)), dma((2,)),
            dma((nz,)), dma((nz,)), dma((2,)), dma((nz,)), dma((nz,)), dma((nz,)), dma,
        ],
        compiler_params=pltpu.CompilerParams(
            collective_id=0, has_side_effects=True, vmem_limit_bytes=60 * 1024 * 1024
        ),
    )(velocity)


def solution(mesh):
    in_specs = (P(None, "gx", "gy", "gz"),)
    out_specs = (
        P("gx", ("gy", "gz"), None),
        P("gx", "gy", None),
        P("gx", "gy", None),
        P("gx", "gy", None),
        P("gx", "gy", None),
        P("gx", "gy", None),
    )
    return jax.shard_map(
        on_device, mesh=mesh, in_specs=in_specs, out_specs=out_specs, check_vma=False
    )
```

```python
import functools

import jax
import jax.numpy as jnp
from jax import lax
from jax.experimental import pallas as pl
from jax.experimental.pallas import tpu as pltpu
from jax.sharding import PartitionSpec as P

MESH = pl.DeviceIdType.MESH
LANES = 128
LOADS = 4


def remote(src, dst, send, recv, device):
    return pltpu.make_async_remote_copy(
        src_ref=src, dst_ref=dst, send_sem=send, recv_sem=recv, device_id=device, device_id_type=MESH
    )


def halves(size, along):
    shape = (size, size // 2) if along else (size // 2, size)
    fine = lax.broadcasted_iota(jnp.int32, shape, 1 - along)
    coarse = lax.broadcasted_iota(jnp.int32, shape, along)
    return jnp.where(fine // 2 == coarse, 1.0, 0.0).astype(jnp.float32)


def dot(a, b):
    return jnp.dot(a, b, precision=lax.Precision.HIGHEST, preferred_element_type=jnp.float32)


def merge(summed):
    rows, depth = summed.shape
    across = dot(summed, halves(depth, 1))
    return dot(halves(rows, 0), across) * 0.125


def kernel(
    sizes, vel_hbm, pencil, one_out, two, three, four, five,
    vel, ypack, yhalo, zpack, zhalo, stage, one, own_one,
    load_sem, xs_sem, xr_sem, ys_sem, yr_sem, zs_sem, zr_sem,
    as_sem, ar_sem, own_sem, up_sem, down_sem, one_sem, store_sem,
):
    nx, ny, nz = sizes
    gx, gy, me = lax.axis_index("gx"), lax.axis_index("gy"), lax.axis_index("gz")
    _, planes, cols, depth = vel_hbm.shape
    rows = cols // nz
    half = depth // 2

    def at(dx=0, dy=0, dz=0):
        return (lax.rem(gx + dx + nx, nx), lax.rem(gy + dy + ny, ny), lax.rem(me + dz + nz, nz))

    barrier = pltpu.get_barrier_semaphore()
    friends = [at(dx=1), at(dx=-1), at(dy=1), at(dy=-1)] + [at(dz=d) for d in range(1, nz)]
    for friend in friends:
        pl.semaphore_signal(barrier, inc=1, device_id=friend, device_id_type=MESH)

    step = planes // LOADS
    loads = []
    for k in range(LOADS):
        loads.append(pltpu.make_async_copy(
            vel_hbm.at[:, pl.ds(k * step, step)], vel.at[:, pl.ds(1 + k * step, step)], load_sem.at[k]))
        loads[-1].start()
    pl.semaphore_wait(barrier, len(friends))

    xcopies = [
        remote(vel_hbm.at[pl.ds(1, 2), planes - 1], vel.at[pl.ds(1, 2), 0], xs_sem.at[0], xr_sem.at[0], at(dx=1)),
        remote(vel_hbm.at[pl.ds(1, 2), 0], vel.at[pl.ds(1, 2), planes + 1], xs_sem.at[1], xr_sem.at[1], at(dx=-1)),
    ]
    for copy in xcopies:
        copy.start()

    lane = lax.broadcasted_iota(jnp.int32, (cols, LANES), 1)

    def pack(x, carry):
        first, last = carry
        for c in range(2):
            first = jnp.where(lane == c * planes + x, vel[c, x + 1, :, 0:1], first)
            last = jnp.where(lane == c * planes + x, vel[c, x + 1, :, depth - 1:depth], last)
            ypack[0, c, pl.ds(x, 1), :] = vel[2 * c, x + 1, 0:1, :]
            ypack[1, c, pl.ds(x, 1), :] = vel[2 * c, x + 1, cols - 1:cols, :]
        return first, last

    carry = (jnp.zeros((cols, LANES), jnp.float32), jnp.zeros((cols, LANES), jnp.float32))
    for k in range(LOADS):
        loads[k].wait()
        carry = lax.fori_loop(k * step, (k + 1) * step, pack, carry)
    zpack[0], zpack[1] = carry
    side = [
        remote(ypack.at[1], yhalo.at[0], ys_sem.at[0], yr_sem.at[0], at(dy=1)),
        remote(ypack.at[0], yhalo.at[1], ys_sem.at[1], yr_sem.at[1], at(dy=-1)),
        remote(zpack.at[1], zhalo.at[0], zs_sem.at[0], zr_sem.at[0], at(dz=1)),
        remote(zpack.at[0], zhalo.at[1], zs_sem.at[1], zr_sem.at[1], at(dz=-1)),
    ]
    for copy in side:
        copy.start()
    for copy in xcopies + side:
        copy.wait_recv()

    row = lax.broadcasted_iota(jnp.int32, (cols, depth), 0)
    deep = lax.broadcasted_iota(jnp.int32, (cols, depth), 1)

    def second(c, x):
        field = vel[2 * c, x + 1]
        ahead = jnp.where(row == cols - 1, yhalo[1, c, pl.ds(x, 1), :], pltpu.roll(field, cols - 1, 0))
        behind = jnp.where(row == 0, yhalo[0, c, pl.ds(x, 1), :], pltpu.roll(field, 1, 0))
        return ahead - behind

    def third(c, x):
        field = vel[c, x + 1]
        shift = LANES - (c * planes + x)
        shift = jnp.where(shift == LANES, 0, shift)
        after = pltpu.roll(zhalo[1], shift, 1)[:, 0:1]
        before = pltpu.roll(zhalo[0], shift, 1)[:, 0:1]
        ahead = jnp.where(deep == depth - 1, after, pltpu.roll(field, depth - 1, 1))
        behind = jnp.where(deep == 0, before, pltpu.roll(field, 1, 1))
        return ahead - behind

    def magnitude(x):
        total = second(1, x) - third(1, x)
        total = total * total
        part = third(0, x) - (vel[2, x + 2] - vel[2, x])
        total = total + part * part
        part = (vel[1, x + 2] - vel[1, x]) - second(0, x)
        total = total + part * part
        return jnp.sqrt(1.0 + 0.25 * total)

    def block(target, first, count):
        here = pl.ds(pl.multiple_of(me * depth, LANES), depth)
        return remote(
            stage.at[target, pl.ds(first, count)], pencil.at[pl.ds(first, count), :, here],
            as_sem.at[target], ar_sem.at[me], (gx, gy, target))

    end = jnp.logical_or(me == 0, me == nz - 1)

    def far(first, count):
        for d in reversed(range(2, nz)):
            @pl.when(me + d < nz)
            def _():
                block(me + d, first, count).start()

            @pl.when(me - d >= 0)
            def _():
                block(me - d, first, count).start()

    def near(first):
        @pl.when(me < nz - 1)
        def _():
            block(me + 1, first, 2).start()

        @pl.when(me > 0)
        def _():
            block(me - 1, first, 2).start()

        @pl.when(jnp.logical_not(end))
        def _():
            far(first, 2)

    def pair(i, carry):
        x = 2 * i
        summed = None
        for k in range(2):
            value = magnitude(x + k)
            for q in range(nz):
                stage[q, x + k] = value[q * rows:(q + 1) * rows, :]
            summed = value if summed is None else summed + value

        @pl.when(i > 0)
        def _():
            near(x - 2)
        own_one[i] = merge(summed)
        return carry

    lax.fori_loop(0, planes // 2, pair, 0)
    near(planes - 2)

    def lanes_of(piece):
        return one.at[:, :, pl.ds(pl.multiple_of(piece * half, LANES), half)]

    def hop(piece, source, up):
        return remote(
            source, lanes_of(piece), (up_sem if up else down_sem).at[piece], one_sem.at[piece],
            (gx, gy, jnp.minimum(me + 1, nz - 1) if up else jnp.maximum(me - 1, 0)))

    @pl.when(me < nz - 1)
    def _():
        hop(me, own_one, True).start()

    @pl.when(me > 0)
    def _():
        hop(me, own_one, False).start()

    @pl.when(end)
    def _():
        far(0, planes)
    keep = pltpu.make_async_copy(
        stage.at[me], pencil.at[:, :, pl.ds(pl.multiple_of(me * depth, LANES), depth)], own_sem.at[0])
    keep.start()
    mine = pltpu.make_async_copy(own_one, lanes_of(me), own_sem.at[1])
    mine.start()

    for k in range(1, nz):
        @pl.when(me - k >= 0)
        def _():
            hop(me - k, own_one, True).wait_recv()

            @pl.when(me < nz - 1)
            def _():
                hop(me - k, lanes_of(me - k), True).start()

        @pl.when(me + k < nz)
        def _():
            hop(me + k, own_one, False).wait_recv()

            @pl.when(me > 0)
            def _():
                hop(me + k, lanes_of(me + k), False).start()
    mine.wait()

    store = pltpu.make_async_copy(one, one_out, store_sem)
    store.start()

    def second_level(i, carry):
        two[i] = merge(one[2 * i] + one[2 * i + 1])
        return carry

    lax.fori_loop(0, two.shape[0], second_level, 0)
    for fine, coarse in ((two, three), (three, four), (four, five)):
        for i in range(coarse.shape[0]):
            coarse[i] = merge(fine[2 * i] + fine[2 * i + 1])
    store.wait()
    keep.wait()
    for copy in xcopies + side:
        copy.wait_send()
    for p in range(nz):
        @pl.when(jnp.logical_and(p <= me, me < nz - 1))
        def _():
            hop(p, own_one, True).wait_send()

        @pl.when(jnp.logical_and(p >= me, me > 0))
        def _():
            hop(p, own_one, False).wait_send()
    for p in range(nz):
        @pl.when(p != me)
        def _():
            block(p, 0, planes).wait_send()
            there = pl.ds(p * depth, depth)
            remote(stage.at[p], pencil.at[:, :, there], as_sem.at[p], ar_sem.at[p], (gx, gy, p)).wait_recv()


def finish(
    pencil_in, one_in, two_in, three_in, four_in, five_in, pencil, one, two, three, four, five,
    pencil_buf, one_buf, two_buf, in_sem, out_sem,
):
    step = pencil_in.shape[0] // LOADS
    moves = [
        (pencil_in.at[pl.ds(k * step, step)], pencil_buf.at[pl.ds(k * step, step)], pencil.at[pl.ds(k * step, step)])
        for k in range(LOADS)
    ] + [(one_in, one_buf, one), (two_in, two_buf, two)]
    loads = [pltpu.make_async_copy(a, b, in_sem.at[i]) for i, (a, b, _) in enumerate(moves)]
    stores = [pltpu.make_async_copy(b, c, out_sem.at[i]) for i, (_, b, c) in enumerate(moves)]
    for load in loads:
        load.start()
    for source, target in ((three_in, three), (four_in, four), (five_in, five)):
        for j in range(target.shape[0]):
            target[j] = source[:, j, :]
    for load, store in zip(loads, stores):
        load.wait()
        store.start()
    for store in stores:
        store.wait()


def on_device(velocity):
    nx, ny, nz = (lax.axis_size(a) for a in ("gx", "gy", "gz"))
    _, planes, cols, depth = velocity.shape
    full = depth * nz
    f32 = jnp.float32

    def level(k):
        return jax.ShapeDtypeStruct((planes >> k, cols >> k, full >> k), f32)

    vmem = pl.BlockSpec(memory_space=pltpu.VMEM)
    anywhere = pl.BlockSpec(memory_space=pl.ANY)
    dma = pltpu.SemaphoreType.DMA
    first = pl.pallas_call(
        functools.partial(kernel, (nx, ny, nz)),
        out_shape=(jax.ShapeDtypeStruct((planes, cols // nz, full), f32),) + tuple(level(k) for k in range(1, 6)),
        in_specs=[anywhere],
        out_specs=(anywhere, anywhere, vmem, vmem, vmem, vmem),
        scratch_shapes=[
            pltpu.VMEM((3, planes + 2, cols, depth), f32),
            pltpu.VMEM((2, 2, planes, depth), f32),
            pltpu.VMEM((2, 2, planes, depth), f32),
            pltpu.VMEM((2, cols, LANES), f32),
            pltpu.VMEM((2, cols, LANES), f32),
            pltpu.VMEM((nz, planes, cols // nz, depth), f32),
            pltpu.VMEM((planes // 2, cols // 2, full // 2), f32),
            pltpu.VMEM((planes // 2, cols // 2, depth // 2), f32),
            dma((LOADS,)), dma((2,)), dma((2,)), dma((2,)), dma((2,)), dma((2,)), dma((2,)),
            dma((nz,)), dma((nz,)), dma((2,)), dma((nz,)), dma((nz,)), dma((nz,)), dma,
        ],
        compiler_params=pltpu.CompilerParams(
            collective_id=0, has_side_effects=True, vmem_limit_bytes=60 * 1024 * 1024
        ),
    )(velocity)
    small = [jax.ShapeDtypeStruct((x.shape[1], x.shape[0], x.shape[2]), f32) for x in first[3:]]
    last = pl.pallas_call(
        finish,
        out_shape=tuple(jax.ShapeDtypeStruct(x.shape, f32) for x in first[:3]) + tuple(small),
        in_specs=[anywhere] * 3 + [vmem] * 3,
        out_specs=(anywhere,) * 3 + (vmem,) * 3,
        scratch_shapes=[pltpu.VMEM(x.shape, f32) for x in first[:3]] + [dma((LOADS + 2,)), dma((LOADS + 2,))],
    )(*first)
    return tuple(last[:3]) + tuple(jnp.transpose(x, (1, 0, 2)) for x in last[3:])


def solution(mesh):
    in_specs = (P(None, "gx", "gy", "gz"),)
    out_specs = (
        P("gx", ("gy", "gz"), None),
        P("gx", "gy", None),
        P("gx", "gy", None),
        P("gx", "gy", None),
        P("gx", "gy", None),
        P("gx", "gy", None),
    )
    return jax.shard_map(
        on_device, mesh=mesh, in_specs=in_specs, out_specs=out_specs, check_vma=False
    )
```

```python
import functools

import jax
import jax.numpy as jnp
from jax import lax
from jax.experimental import pallas as pl
from jax.experimental.pallas import tpu as pltpu
from jax.sharding import PartitionSpec as P

MESH = pl.DeviceIdType.MESH
LANES = 128
LOADS = 4


def remote(src, dst, send, recv, device):
    return pltpu.make_async_remote_copy(
        src_ref=src, dst_ref=dst, send_sem=send, recv_sem=recv, device_id=device, device_id_type=MESH
    )


def halves(size, along):
    shape = (size, size // 2) if along else (size // 2, size)
    fine = lax.broadcasted_iota(jnp.int32, shape, 1 - along)
    coarse = lax.broadcasted_iota(jnp.int32, shape, along)
    return jnp.where(fine // 2 == coarse, 1.0, 0.0).astype(jnp.float32)


def dot(a, b):
    return jnp.dot(a, b, precision=lax.Precision.HIGHEST, preferred_element_type=jnp.float32)


def merge(summed):
    rows, depth = summed.shape
    across = dot(summed, halves(depth, 1))
    return dot(halves(rows, 0), across) * 0.125


def kernel(
    sizes, vel_hbm, pencil, one_out, two, three, four, five,
    vel, ypack, yhalo, zpack, zhalo, stage, one, own_one,
    load_sem, xs_sem, xr_sem, ys_sem, yr_sem, zs_sem, zr_sem,
    as_sem, ar_sem, own_sem, up_sem, down_sem, one_sem, store_sem,
):
    nx, ny, nz = sizes
    gx, gy, me = lax.axis_index("gx"), lax.axis_index("gy"), lax.axis_index("gz")
    _, planes, cols, depth = vel_hbm.shape
    rows = cols // nz
    half = depth // 2

    def at(dx=0, dy=0, dz=0):
        return (lax.rem(gx + dx + nx, nx), lax.rem(gy + dy + ny, ny), lax.rem(me + dz + nz, nz))

    barrier = pltpu.get_barrier_semaphore()
    friends = [at(dx=1), at(dx=-1), at(dy=1), at(dy=-1)] + [at(dz=d) for d in range(1, nz)]
    for friend in friends:
        pl.semaphore_signal(barrier, inc=1, device_id=friend, device_id_type=MESH)

    step = planes // LOADS
    loads = []
    for k in range(LOADS):
        loads.append(pltpu.make_async_copy(
            vel_hbm.at[:, pl.ds(k * step, step)], vel.at[:, pl.ds(1 + k * step, step)], load_sem.at[k]))
        loads[-1].start()
    pl.semaphore_wait(barrier, len(friends))

    xcopies = [
        remote(vel_hbm.at[pl.ds(1, 2), planes - 1], vel.at[pl.ds(1, 2), 0], xs_sem.at[0], xr_sem.at[0], at(dx=1)),
        remote(vel_hbm.at[pl.ds(1, 2), 0], vel.at[pl.ds(1, 2), planes + 1], xs_sem.at[1], xr_sem.at[1], at(dx=-1)),
    ]
    for copy in xcopies:
        copy.start()

    lane = lax.broadcasted_iota(jnp.int32, (cols, LANES), 1)

    def pack(x, carry):
        first, last = carry
        for c in range(2):
            first = jnp.where(lane == c * planes + x, vel[c, x + 1, :, 0:1], first)
            last = jnp.where(lane == c * planes + x, vel[c, x + 1, :, depth - 1:depth], last)
            ypack[0, c, pl.ds(x, 1), :] = vel[2 * c, x + 1, 0:1, :]
            ypack[1, c, pl.ds(x, 1), :] = vel[2 * c, x + 1, cols - 1:cols, :]
        return first, last

    carry = (jnp.zeros((cols, LANES), jnp.float32), jnp.zeros((cols, LANES), jnp.float32))
    for k in range(LOADS):
        loads[k].wait()
        carry = lax.fori_loop(k * step, (k + 1) * step, pack, carry)
    zpack[0], zpack[1] = carry
    side = [
        remote(ypack.at[1], yhalo.at[0], ys_sem.at[0], yr_sem.at[0], at(dy=1)),
        remote(ypack.at[0], yhalo.at[1], ys_sem.at[1], yr_sem.at[1], at(dy=-1)),
        remote(zpack.at[1], zhalo.at[0], zs_sem.at[0], zr_sem.at[0], at(dz=1)),
        remote(zpack.at[0], zhalo.at[1], zs_sem.at[1], zr_sem.at[1], at(dz=-1)),
    ]
    for copy in side:
        copy.start()
    for copy in xcopies + side:
        copy.wait_recv()

    row = lax.broadcasted_iota(jnp.int32, (cols, depth), 0)
    deep = lax.broadcasted_iota(jnp.int32, (cols, depth), 1)

    def second(c, x):
        field = vel[2 * c, x + 1]
        ahead = jnp.where(row == cols - 1, yhalo[1, c, pl.ds(x, 1), :], pltpu.roll(field, cols - 1, 0))
        behind = jnp.where(row == 0, yhalo[0, c, pl.ds(x, 1), :], pltpu.roll(field, 1, 0))
        return ahead - behind

    def third(c, x):
        field = vel[c, x + 1]
        shift = LANES - (c * planes + x)
        shift = jnp.where(shift == LANES, 0, shift)
        after = pltpu.roll(zhalo[1], shift, 1)[:, 0:1]
        before = pltpu.roll(zhalo[0], shift, 1)[:, 0:1]
        ahead = jnp.where(deep == depth - 1, after, pltpu.roll(field, depth - 1, 1))
        behind = jnp.where(deep == 0, before, pltpu.roll(field, 1, 1))
        return ahead - behind

    def magnitude(x):
        total = second(1, x) - third(1, x)
        total = total * total
        part = third(0, x) - (vel[2, x + 2] - vel[2, x])
        total = total + part * part
        part = (vel[1, x + 2] - vel[1, x]) - second(0, x)
        total = total + part * part
        return jnp.sqrt(1.0 + 0.25 * total)

    def block(target, first, count):
        here = pl.ds(pl.multiple_of(me * depth, LANES), depth)
        return remote(
            stage.at[target, pl.ds(first, count)], pencil.at[pl.ds(first, count), :, here],
            as_sem.at[target], ar_sem.at[me], (gx, gy, target))

    end = jnp.logical_or(me == 0, me == nz - 1)

    def far(first, count):
        for d in reversed(range(2, nz)):
            @pl.when(me + d < nz)
            def _():
                block(me + d, first, count).start()

            @pl.when(me - d >= 0)
            def _():
                block(me - d, first, count).start()

    def near(first):
        @pl.when(me < nz - 1)
        def _():
            block(me + 1, first, 2).start()

        @pl.when(me > 0)
        def _():
            block(me - 1, first, 2).start()

    def pair(i, carry):
        x = 2 * i
        summed = None
        for k in range(2):
            value = magnitude(x + k)
            for q in range(nz):
                stage[q, x + k] = value[q * rows:(q + 1) * rows, :]
            summed = value if summed is None else summed + value

        @pl.when(i > 0)
        def _():
            near(x - 2)
        own_one[i] = merge(summed)
        return carry

    lax.fori_loop(0, planes // 2, pair, 0)
    near(planes - 2)

    def lanes_of(piece):
        return one.at[:, :, pl.ds(pl.multiple_of(piece * half, LANES), half)]

    def hop(piece, source, up):
        return remote(
            source, lanes_of(piece), (up_sem if up else down_sem).at[piece], one_sem.at[piece],
            (gx, gy, jnp.minimum(me + 1, nz - 1) if up else jnp.maximum(me - 1, 0)))

    @pl.when(me < nz - 1)
    def _():
        hop(me, own_one, True).start()

    @pl.when(me > 0)
    def _():
        hop(me, own_one, False).start()

    @pl.when(end)
    def _():
        far(0, planes)
    keep = pltpu.make_async_copy(
        stage.at[me], pencil.at[:, :, pl.ds(pl.multiple_of(me * depth, LANES), depth)], own_sem.at[0])
    keep.start()
    mine = pltpu.make_async_copy(own_one, lanes_of(me), own_sem.at[1])
    mine.start()

    for k in range(1, nz):
        @pl.when(me - k >= 0)
        def _():
            hop(me - k, own_one, True).wait_recv()

            @pl.when(me < nz - 1)
            def _():
                hop(me - k, lanes_of(me - k), True).start()

        @pl.when(me + k < nz)
        def _():
            hop(me + k, own_one, False).wait_recv()

            @pl.when(me > 0)
            def _():
                hop(me + k, lanes_of(me + k), False).start()
        if k == 1:
            @pl.when(jnp.logical_not(end))
            def _():
                far(0, planes)
    mine.wait()

    store = pltpu.make_async_copy(one, one_out, store_sem)
    store.start()

    def second_level(i, carry):
        two[i] = merge(one[2 * i] + one[2 * i + 1])
        return carry

    lax.fori_loop(0, two.shape[0], second_level, 0)
    for fine, coarse in ((two, three), (three, four), (four, five)):
        for i in range(coarse.shape[0]):
            coarse[i] = merge(fine[2 * i] + fine[2 * i + 1])
    store.wait()
    keep.wait()
    for copy in xcopies + side:
        copy.wait_send()
    for p in range(nz):
        @pl.when(jnp.logical_and(p <= me, me < nz - 1))
        def _():
            hop(p, own_one, True).wait_send()

        @pl.when(jnp.logical_and(p >= me, me > 0))
        def _():
            hop(p, own_one, False).wait_send()
    for p in range(nz):
        @pl.when(p != me)
        def _():
            block(p, 0, planes).wait_send()
            there = pl.ds(p * depth, depth)
            remote(stage.at[p], pencil.at[:, :, there], as_sem.at[p], ar_sem.at[p], (gx, gy, p)).wait_recv()


def finish(
    pencil_in, one_in, two_in, three_in, four_in, five_in, pencil, one, two, three, four, five,
    pencil_buf, one_buf, two_buf, in_sem, out_sem,
):
    step = pencil_in.shape[0] // LOADS
    moves = [
        (pencil_in.at[pl.ds(k * step, step)], pencil_buf.at[pl.ds(k * step, step)], pencil.at[pl.ds(k * step, step)])
        for k in range(LOADS)
    ] + [(one_in, one_buf, one), (two_in, two_buf, two)]
    loads = [pltpu.make_async_copy(a, b, in_sem.at[i]) for i, (a, b, _) in enumerate(moves)]
    stores = [pltpu.make_async_copy(b, c, out_sem.at[i]) for i, (_, b, c) in enumerate(moves)]
    for load in loads:
        load.start()
    for source, target in ((three_in, three), (four_in, four), (five_in, five)):
        for j in range(target.shape[0]):
            target[j] = source[:, j, :]
    for load, store in zip(loads, stores):
        load.wait()
        store.start()
    for store in stores:
        store.wait()


def on_device(velocity):
    nx, ny, nz = (lax.axis_size(a) for a in ("gx", "gy", "gz"))
    _, planes, cols, depth = velocity.shape
    full = depth * nz
    f32 = jnp.float32

    def level(k):
        return jax.ShapeDtypeStruct((planes >> k, cols >> k, full >> k), f32)

    vmem = pl.BlockSpec(memory_space=pltpu.VMEM)
    anywhere = pl.BlockSpec(memory_space=pl.ANY)
    dma = pltpu.SemaphoreType.DMA
    first = pl.pallas_call(
        functools.partial(kernel, (nx, ny, nz)),
        out_shape=(jax.ShapeDtypeStruct((planes, cols // nz, full), f32),) + tuple(level(k) for k in range(1, 6)),
        in_specs=[anywhere],
        out_specs=(anywhere, anywhere, vmem, vmem, vmem, vmem),
        scratch_shapes=[
            pltpu.VMEM((3, planes + 2, cols, depth), f32),
            pltpu.VMEM((2, 2, planes, depth), f32),
            pltpu.VMEM((2, 2, planes, depth), f32),
            pltpu.VMEM((2, cols, LANES), f32),
            pltpu.VMEM((2, cols, LANES), f32),
            pltpu.VMEM((nz, planes, cols // nz, depth), f32),
            pltpu.VMEM((planes // 2, cols // 2, full // 2), f32),
            pltpu.VMEM((planes // 2, cols // 2, depth // 2), f32),
            dma((LOADS,)), dma((2,)), dma((2,)), dma((2,)), dma((2,)), dma((2,)), dma((2,)),
            dma((nz,)), dma((nz,)), dma((2,)), dma((nz,)), dma((nz,)), dma((nz,)), dma,
        ],
        compiler_params=pltpu.CompilerParams(
            collective_id=0, has_side_effects=True, vmem_limit_bytes=60 * 1024 * 1024
        ),
    )(velocity)
    small = [jax.ShapeDtypeStruct((x.shape[1], x.shape[0], x.shape[2]), f32) for x in first[3:]]
    last = pl.pallas_call(
        finish,
        out_shape=tuple(jax.ShapeDtypeStruct(x.shape, f32) for x in first[:3]) + tuple(small),
        in_specs=[anywhere] * 3 + [vmem] * 3,
        out_specs=(anywhere,) * 3 + (vmem,) * 3,
        scratch_shapes=[pltpu.VMEM(x.shape, f32) for x in first[:3]] + [dma((LOADS + 2,)), dma((LOADS + 2,))],
    )(*first)
    return tuple(last[:3]) + tuple(jnp.transpose(x, (1, 0, 2)) for x in last[3:])


def solution(mesh):
    in_specs = (P(None, "gx", "gy", "gz"),)
    out_specs = (
        P("gx", ("gy", "gz"), None),
        P("gx", "gy", None),
        P("gx", "gy", None),
        P("gx", "gy", None),
        P("gx", "gy", None),
        P("gx", "gy", None),
    )
    return jax.shard_map(
        on_device, mesh=mesh, in_specs=in_specs, out_specs=out_specs, check_vma=False
    )
```
